256 devices in a mesh: row: 4 (over y_lo, core), col: 64 (over z, y_hi, x).
Axes of the slice: x: 4, y: 4 (y_hi: 2, y_lo: 2; y = y_hi * 2 + y_lo), z: 8, core: 2. Of those that a mesh axis runs over, the one named last changes fastest.
Arguments:
- image: bfloat16 [8192, 1024], P(('col', 'row')), may hold values from -1 to 1
- text: bfloat16 [8192, 1024], P(('row', 'col')), may hold values from -1 to 1
- audio: bfloat16 [8192, 1024], P(('row', 'col')), may hold values from -1 to 1
Outputs:
- image_grad: float32 [8192, 1024], P(('col', 'row'))
- text_grad: float32 [8192, 1024], P(('row', 'col'))
- audio_grad: float32 [8192, 1024], P(('row', 'col'))
- loss: float32 [], replicated
The draws below stay inside these ranges and needn't reach their ends.
All inputs are finite; a program needn't handle non-finite values.
Results may differ from the reference program's by a relative error of at most 0.0063.
Values may be sent and summed in bfloat16 or wider, within the bound.
No kernel may reach another device: no remote copies, remote signals or barrier semaphores. Data moves between devices by JAX's collectives and lax.ppermute only.
A program may use at most 64 MiB of HBM per device.

```python
import math
import jax
import jax.numpy as jnp
from jax import lax

E = 1024
BATCH = 8192


def common_rows(key):
    base_key = jax.random.fold_in(key, 7001)
    direction = jax.random.normal(jax.random.fold_in(base_key, 1), (BATCH, E), jnp.float32)
    return direction


def row_scales(own_key):
    lower, upper = (0.5, 2.0)
    logs = jax.random.uniform(jax.random.fold_in(own_key, 11), (BATCH, 1), jnp.float32, math.log(lower), math.log(upper))
    return jnp.exp(logs)


def paired_rows(key, stream):
    direction = common_rows(key)
    own_key = jax.random.fold_in(key, stream)
    mixing = jax.random.uniform(jax.random.fold_in(own_key, 5), (BATCH, 1), jnp.float32, 0.25, 0.85)
    own_noise = jax.random.normal(jax.random.fold_in(own_key, 6), (BATCH, E), jnp.float32)
    mixed = mixing * direction + jnp.sqrt(1.0 - mixing * mixing) * own_noise
    values = mixed * row_scales(own_key) * 0.03125
    return jnp.clip(values, -1.0, 1.0).astype(jnp.bfloat16)


def draw_image(key, part):
    direction = common_rows(key)
    own_key = jax.random.fold_in(key, 8101)
    values = direction * row_scales(own_key) * 0.03125
    return jnp.clip(values, -1.0, 1.0).astype(jnp.bfloat16)


def draw_text(key, part):
    return paired_rows(key, 8202)


def draw_audio(key, part):
    return paired_rows(key, 8303)


def setup_inputs(seed: int = 0) -> dict:
    splits = jax.random.split(jax.random.key(seed), 4)
    return {
        "image": draw_image(jax.random.fold_in(splits[3], 71), 0),
        "text": draw_text(jax.random.fold_in(splits[3], 71), 0),
        "audio": draw_audio(jax.random.fold_in(splits[3], 71), 0),
    }


logit_scale = 20.0
epsilon = 1e-06

def normalize(values):
    widened = values.astype(jnp.float32)
    radius = jnp.sqrt(lax.optimization_barrier(jnp.sum(widened * widened, axis=-1, keepdims=True)) + epsilon)
    return (widened / radius, radius)

def through_norm(grad_unit, unit, radius):
    inner = lax.optimization_barrier(jnp.sum(unit * grad_unit, axis=-1, keepdims=True))
    return (grad_unit - unit * inner) / radius

def scores(left, right):
    return logit_scale * lax.dot_general(left, right, (((1,), (1,)), ((), ())), preferred_element_type=jnp.float32)

def reference(image, text, audio):
    batch_size = image.shape[0]
    feature_width = image.shape[1]
    block_rows = min(512, batch_size)
    block_count = batch_size // block_rows
    image_unit, image_radius = normalize(image)
    text_unit, text_radius = normalize(text)
    audio_unit, audio_radius = normalize(audio)
    image_half = image_unit.astype(jnp.bfloat16)
    text_half = text_unit.astype(jnp.bfloat16)
    audio_half = audio_unit.astype(jnp.bfloat16)
    blocks = jnp.arange(block_count, dtype=jnp.int32)

    def first_pass(running, block_index):
        image_rows = lax.dynamic_slice_in_dim(image_half, block_index * block_rows, block_rows, 0)
        text_exp = jnp.exp(scores(image_rows, text_half) - logit_scale)
        audio_exp = jnp.exp(scores(image_rows, audio_half) - logit_scale)
        updated = (running[0] + lax.optimization_barrier(jnp.sum(text_exp, axis=0)), running[1] + lax.optimization_barrier(jnp.sum(audio_exp, axis=0)))
        return (updated, (lax.optimization_barrier(jnp.sum(text_exp, axis=1)), lax.optimization_barrier(jnp.sum(audio_exp, axis=1))))
    empty_sums = jnp.zeros((batch_size,), jnp.float32)
    (text_column, audio_column), (text_row, audio_row) = lax.scan(first_pass, (empty_sums, empty_sums), blocks)
    text_row = text_row.reshape(batch_size)
    audio_row = audio_row.reshape(batch_size)
    positions = jnp.arange(batch_size, dtype=jnp.int32)

    def second_pass(running, block_index):
        first_row = (block_index * block_rows).astype(jnp.int32)
        image_rows = lax.dynamic_slice_in_dim(image_half, first_row, block_rows, 0)
        diagonal = (first_row + jnp.arange(block_rows, dtype=jnp.int32))[:, None] == positions[None, :]
        twice_diagonal = jnp.where(diagonal, 2.0, 0.0).astype(jnp.float32)
        text_scores = scores(image_rows, text_half)
        audio_scores = scores(image_rows, audio_half)
        text_exp = jnp.exp(text_scores - logit_scale)
        audio_exp = jnp.exp(audio_scores - logit_scale)
        row_text = lax.dynamic_slice_in_dim(text_row, first_row, block_rows, 0)
        row_audio = lax.dynamic_slice_in_dim(audio_row, first_row, block_rows, 0)
        text_weights = (text_exp / row_text[:, None] + text_exp / text_column[None, :] - twice_diagonal).astype(jnp.bfloat16)
        audio_weights = (audio_exp / row_audio[:, None] + audio_exp / audio_column[None, :] - twice_diagonal).astype(jnp.bfloat16)
        image_part = logit_scale * (jnp.dot(text_weights, text_half, preferred_element_type=jnp.float32) + jnp.dot(audio_weights, audio_half, preferred_element_type=jnp.float32))
        text_acc = running[0] + lax.dot_general(text_weights, image_rows, (((0,), (0,)), ((), ())), preferred_element_type=jnp.float32)
        audio_acc = running[1] + lax.dot_general(audio_weights, image_rows, (((0,), (0,)), ((), ())), preferred_element_type=jnp.float32)
        diagonal_sum = running[2] + jnp.sum(jnp.where(diagonal, text_scores + audio_scores, 0.0))
        return ((text_acc, audio_acc, diagonal_sum), image_part)
    empty_grad = jnp.zeros((batch_size, feature_width), jnp.float32)
    (text_acc, audio_acc, diagonal_sum), image_part = lax.scan(second_pass, (empty_grad, empty_grad, jnp.zeros((), jnp.float32)), blocks)
    image_part = image_part.reshape(batch_size, feature_width)
    loss_sum = jnp.sum(jnp.log(text_row)) + jnp.sum(jnp.log(audio_row)) + jnp.sum(jnp.log(text_column)) + jnp.sum(jnp.log(audio_column)) - 2.0 * diagonal_sum
    loss = loss_sum / (4.0 * batch_size) + logit_scale
    return (through_norm(image_part, image_unit, image_radius), through_norm(logit_scale * text_acc, text_unit, text_radius), through_norm(logit_scale * audio_acc, audio_unit, audio_radius), loss)
```

```python
import jax
import jax.numpy as jnp
from jax import lax
from jax.sharding import Mesh
from jax.sharding import PartitionSpec as P

AXES = ("y_lo", "core", "z", "y_hi", "x")
COL_ROW = ("z", "y_hi", "x", "y_lo", "core")

logit_scale = 20.0
epsilon = 1e-06


def place(core, x, y, z):
    return (((y % 4 % 2 * 2 + core % 2) * 8 + z % 8) * 2 + y % 4 // 2) * 4 + x % 4


def send(array, move):
    pairs = [
        (place(core, x, y, z), place(*move(core, x, y, z)))
        for core in range(2)
        for x in range(4)
        for y in range(4)
        for z in range(8)
    ]
    return lax.ppermute(array, AXES, pairs)


def swap(array):
    return send(array, lambda core, x, y, z: (1 - core, x, y, z))


def along_first(array, k):
    return send(
        array, lambda core, x, y, z: (core, x, y + k, z) if core else (core, x + k, y, z)
    )


def along_second(array, k):
    return send(
        array, lambda core, x, y, z: (core, x + k, y, z) if core else (core, x, y + k, z)
    )


def along_z(array, k):
    return send(array, lambda core, x, y, z: (core, x, y, z - k if core else z + k))


def up_z(array, k):
    return send(array, lambda core, x, y, z: (core, x, y, z + k))


def normalize(values):
    widened = values.astype(jnp.float32)
    radius = jnp.sqrt(jnp.sum(widened * widened, axis=-1, keepdims=True) + epsilon)
    return (widened / radius, radius)


def through_norm(grad_unit, unit, radius):
    inner = jnp.sum(unit * grad_unit, axis=-1, keepdims=True)
    return (grad_unit - unit * inner) / radius


def dot(left, right, contract):
    return lax.dot_general(left, right, (contract, ((), ())), preferred_element_type=jnp.float32)


def pieces(value, width):
    high = value.astype(jnp.bfloat16).astype(jnp.float32)
    rest = value - high
    middle = rest.astype(jnp.bfloat16).astype(jnp.float32)
    lane = lax.broadcasted_iota(jnp.int32, (8, width), 1)
    return jnp.where(
        lane == 0, high, jnp.where(lane == 1, middle, jnp.where(lane == 2, rest - middle, 0.0))
    ).astype(jnp.bfloat16)


def whole(row):
    return jnp.sum(row[:1, :3].astype(jnp.float32))


def sum_z(rows, plain):
    both = jnp.concatenate([rows, plain], axis=1)
    n = rows.shape[1]

    def turned(got, k):
        return jnp.concatenate([jnp.roll(got[:, :n], -k, axis=0), got[:, n:]], axis=1)

    below, above = up_z(both, 1), up_z(both, -1)
    lower = both + turned(below, 1)
    three = lower + turned(above, -1)
    far_below, far_above = up_z(three, 3), up_z(lower, -3)
    return three + turned(far_below, 3) + turned(far_above, -3)


def sum_plane(parts):
    got = [along_first(parts, k) for k in (1, 3, 2)]
    parts = parts + sum(jnp.roll(g, k, axis=1) for g, k in zip(got, (1, 3, 2)))
    got = [along_second(parts, k) for k in (1, 3, 2)]
    return parts + sum(jnp.roll(g, k, axis=0) for g, k in zip(got, (1, 3, 2)))


def shards(image, text, audio):
    rows = image.shape[0]
    width = image.shape[1]
    core, z, x = lax.axis_index("core"), lax.axis_index("z"), lax.axis_index("x")
    y_lo, y_hi = lax.axis_index("y_lo"), lax.axis_index("y_hi")
    y = y_hi * 2 + y_lo
    first = core == 0

    def ordered(mine, other):
        return jnp.where(
            first, jnp.concatenate([mine, other]), jnp.concatenate([other, mine])
        )

    def own(pair):
        return jnp.where(first, pair[:rows], pair[rows:])

    def partners(pair):
        return jnp.where(first, pair[rows:], pair[:rows])

    image_unit, image_radius = normalize(image)
    text_unit, text_radius = normalize(text)
    audio_unit, audio_radius = normalize(audio)
    image_half = image_unit.astype(jnp.bfloat16)
    text_half = text_unit.astype(jnp.bfloat16)
    audio_half = audio_unit.astype(jnp.bfloat16)

    got = swap(jnp.concatenate([image_half, jnp.where(first, audio_half, text_half)]))
    image_pair = ordered(image_half, got[:rows])
    other_pair = ordered(jnp.where(first, text_half, audio_half), got[rows:])

    near = {k: along_first(other_pair, k) for k in (1, 3, 2)}
    line = jnp.concatenate([other_pair, near[1], near[2], near[3]])
    ups = {4: along_z(image_half, 4)}
    ups.update({k: along_z(image_pair, k) for k in (3, 2, 1)})
    far = {k: along_second(line, k) for k in (1, 3, 2)}
    here = jnp.concatenate([ups[1], ups[2], ups[3], ups[4]])
    image_tile = jnp.concatenate([image_pair, here, swap(here)])
    other_tile = jnp.concatenate([line, far[1], far[2], far[3]])

    half = jnp.arange(2)
    steps = jnp.array([1, 1, 2, 2, 3, 3, 4])
    toward = jnp.where(first, -1, 1)
    image_z = jnp.concatenate([jnp.zeros(2, jnp.int32), steps * toward, -steps * toward]) + z
    image_core = jnp.concatenate([half, half, half, half, core[None], half, half, half, 1 - core[None]])
    image_block = image_z % 8 * 32 + y_hi * 16 + x * 4 + y_lo * 2 + image_core
    a, b = jnp.arange(32) // 2 % 4, jnp.arange(32) // 8
    other_x = (x - jnp.where(first, a, b)) % 4
    other_y = (y - jnp.where(first, b, a)) % 4
    other_block = (
        other_y % 2 * 128 + jnp.arange(32) % 2 * 64 + z * 8 + other_y // 2 * 4 + other_x
    )
    inside = jnp.arange(rows)
    image_ids = (image_block[:, None] * rows + inside[None, :]).reshape(-1)
    other_ids = (other_block[:, None] * rows + inside[None, :]).reshape(-1)
    diagonal = image_ids[:, None] == other_ids[None, :]

    scores = logit_scale * dot(image_tile, other_tile, ((1,), (1,)))
    exps = jnp.exp(scores - logit_scale)
    row_part, column_part = jnp.sum(exps, axis=1), jnp.sum(exps, axis=0)
    matched = jnp.sum(jnp.where(diagonal, scores, 0.0))

    pair = 2 * rows
    head, mine, others = row_part[:pair], row_part[pair : 9 * rows], row_part[9 * rows :]
    lower, upper = jnp.where(first, mine, others), jnp.where(first, others, mine)

    def split(v):
        return v[:pair], v[pair : 2 * pair], v[2 * pair : 3 * pair], v[3 * pair :]

    d1, d2, d3, d4 = split(lower)
    u1, u2, u3, u4 = split(upper)
    cycle = jnp.concatenate([head, u1, u2, u3, d4, u4, d3, d2, d1]).reshape(8, pair)
    summed = sum_z(cycle, jnp.broadcast_to(matched, (8, pair)))
    matched = summed[0, pair]
    cycle = summed[:, :pair]
    lower = jnp.concatenate([cycle[7], cycle[6], cycle[5], cycle[4, :rows]])
    upper = jnp.concatenate([cycle[1], cycle[2], cycle[3], cycle[4, rows:]])
    row_total = jnp.concatenate(
        [cycle[0], jnp.where(first, lower, upper), jnp.where(first, upper, lower)]
    )
    column_total = sum_plane(column_part.reshape(4, 4, pair)).reshape(-1)

    weights = (
        exps / row_total[:, None]
        + exps / column_total[None, :]
        - jnp.where(diagonal, 2.0, 0.0)
    ).astype(jnp.bfloat16)

    row_logs = jnp.sum(jnp.log(row_total)) - 2.0 * matched
    column_logs = jnp.sum(jnp.log(column_total))

    image_part = dot(weights, other_tile, ((1,), (0,)))
    other_part = dot(weights, image_tile, ((0,), (0,)))

    got = swap(
        jnp.concatenate(
            [
                partners(image_part[:pair]).astype(jnp.bfloat16),
                image_part[9 * rows :].astype(jnp.bfloat16),
                pieces(column_logs, width),
            ]
        )
    )
    column_logs = column_logs + whole(got[8 * rows :])
    chip = jnp.concatenate([own(image_part[:pair]), image_part[pair : 9 * rows]]) + got[
        : 8 * rows
    ].astype(jnp.float32)
    note = pieces(column_logs, width)
    ends = {1: (1, 3), 2: (3, 5), 3: (5, 7), 4: (7, 8)}
    back = {
        k: along_z(
            jnp.concatenate([chip[ends[k][0] * rows : ends[k][1] * rows].astype(jnp.bfloat16), note]), -k
        )
        for k in (4, 3, 2, 1)
    }

    note = pieces(row_logs, width)
    bundle = 4 * pair
    got = {
        k: along_second(
            jnp.concatenate([other_part[k * bundle : (k + 1) * bundle].astype(jnp.bfloat16), note]), -k
        )
        for k in (1, 3, 2)
    }
    row_logs = row_logs + sum(whole(got[k][bundle:]) for k in (1, 2, 3))
    line = other_part[:bundle] + sum(got[k][:bundle].astype(jnp.float32) for k in (1, 2, 3))
    note = pieces(row_logs, width)
    got = {
        k: along_first(
            jnp.concatenate([line[k * pair : (k + 1) * pair].astype(jnp.bfloat16), note]), -k
        )
        for k in (1, 3, 2)
    }
    row_logs = row_logs + sum(whole(got[k][pair:]) for k in (1, 2, 3))
    other_sum = line[:pair] + sum(got[k][:pair].astype(jnp.float32) for k in (1, 2, 3))

    near = sum(back[k][:pair].astype(jnp.float32) for k in (1, 2, 3))
    image_sum = chip[:rows] + own(near) + back[4][:rows].astype(jnp.float32)
    logs = row_logs + sum(whole(back[k][pair:]) for k in (1, 2, 3))
    logs = logs + jnp.where(first, column_logs + whole(back[4][rows:]), 0.0)
    got = swap(
        jnp.concatenate(
            [
                partners(near).astype(jnp.bfloat16),
                partners(other_sum).astype(jnp.bfloat16),
                pieces(logs, width),
            ]
        )
    )
    image_sum = image_sum + got[:rows].astype(jnp.float32)
    mine, other = own(other_sum), got[rows:pair].astype(jnp.float32)
    text_sum, audio_sum = jnp.where(first, mine, other), jnp.where(first, other, mine)
    batch_size = rows * 256
    loss = (logs + whole(got[pair:])) / (4.0 * batch_size) + logit_scale
    return (
        through_norm(logit_scale * image_sum, image_unit, image_radius),
        through_norm(logit_scale * text_sum, text_unit, text_radius),
        through_norm(logit_scale * audio_sum, audio_unit, audio_radius),
        loss,
    )


def solution(mesh):
    split = Mesh(mesh.devices.reshape(2, 2, 8, 2, 4), AXES)
    image_spec, other_spec = P(COL_ROW, None), P(AXES, None)
    return jax.shard_map(
        shards,
        mesh=split,
        in_specs=(image_spec, other_spec, other_spec),
        out_specs=(image_spec, other_spec, other_spec, P()),
        check_vma=False,
    )
```

```python
import jax
import jax.numpy as jnp
from jax import lax
from jax.experimental import pallas as pl
from jax.experimental.pallas import tpu as pltpu
from jax.sharding import Mesh
from jax.sharding import PartitionSpec as P

AXES = ("y_lo", "core", "z", "y_hi", "x")
COL_ROW = ("z", "y_hi", "x", "y_lo", "core")

logit_scale = 20.0
epsilon = 1e-06
NOTE = 16
CHUNK = 128


def place(core, x, y, z):
    return (((y % 4 % 2 * 2 + core % 2) * 8 + z % 8) * 2 + y % 4 // 2) * 4 + x % 4


def send(array, move):
    pairs = [
        (place(core, x, y, z), place(*move(core, x, y, z)))
        for core in range(2)
        for x in range(4)
        for y in range(4)
        for z in range(8)
    ]
    return lax.ppermute(array, AXES, pairs)


def swap(array):
    return send(array, lambda core, x, y, z: (1 - core, x, y, z))


def along_first(array, k):
    return send(array, lambda core, x, y, z: (core, x, y + k, z) if core else (core, x + k, y, z))


def along_second(array, k):
    return send(array, lambda core, x, y, z: (core, x + k, y, z) if core else (core, x, y + k, z))


def up(array, k):
    return send(array, lambda core, x, y, z: (core, x, y, z - k if core else z + k))


def call(kernel, count, *shapes, last=False, outside=False):
    def space(shape, dtype):
        return jax.ShapeDtypeStruct(shape, dtype) if last else pltpu.VMEM(shape, dtype)

    made = pl.pallas_call(
        kernel,
        out_shape=tuple(space(s, d) for s, d in shapes),
        in_specs=[pl.BlockSpec(memory_space=pltpu.VMEM)] * count,
        out_specs=tuple(pl.BlockSpec(memory_space=pltpu.VMEM) for _ in shapes),
        compiler_params=pltpu.CompilerParams(vmem_limit_bytes=20 * 1024 * 1024),
    )

    def run(*arrays):
        kept_in = pltpu.HBM if outside else pltpu.VMEM
        return made(*(pltpu.with_memory_space_constraint(a, kept_in) for a in arrays))

    return run


def wide(values):
    return values.astype(jnp.float32)


def slim(values):
    return values.astype(jnp.bfloat16)


def normalize(values):
    widened = wide(values)
    radius = jnp.sqrt(jnp.sum(widened * widened, axis=-1, keepdims=True) + epsilon)
    return (widened / radius, radius)


def dot(left, right, contract):
    return lax.dot_general(left, right, (contract, ((), ())), preferred_element_type=jnp.float32)


def pieces(value, width):
    value = jnp.broadcast_to(value, (NOTE, width))
    high = wide(slim(value))
    rest = value - high
    middle = wide(slim(rest))
    lane = lax.broadcasted_iota(jnp.int32, (NOTE, width), 1)
    split = jnp.where(lane == 0, high, jnp.where(lane == 1, middle, rest - middle))
    return slim(jnp.where(lane < 3, split, 0.0))


def whole(rows):
    return jnp.sum(wide(rows)[:1, :128], axis=1, keepdims=True)


def position():
    core, z, x = lax.axis_index("core"), lax.axis_index("z"), lax.axis_index("x")
    return core, x, lax.axis_index("y_hi") * 2 + lax.axis_index("y_lo"), z


def image_ids(at, first_row, count, rows):
    core, x, y, z = at
    r = first_row + lax.broadcasted_iota(jnp.int32, (count, 1), 0)
    block = r // rows
    at_z = (z + jnp.where(core == 0, block // 2, 8 - block // 2)) % 8
    where = at_z * 32 + y // 2 * 16 + x * 4 + y % 2 * 2 + block % 2
    return where * rows + r % rows


def other_ids(at, count, rows):
    core, x, y, z = at
    r = lax.broadcasted_iota(jnp.int32, (1, count), 1)
    block = r // rows
    a, b = block // 2 % 4, block // 8
    at_x = (x - jnp.where(core == 0, a, b) + 4) % 4
    at_y = (y - jnp.where(core == 0, b, a) + 4) % 4
    where = at_y % 2 * 128 + block % 2 * 64 + z * 8 + at_y // 2 * 4 + at_x
    return where * rows + r % rows


def ordered(core, mine, other):
    return jnp.where(core == 0, mine, other), jnp.where(core == 0, other, mine)


def begin_kernel(rows, image, text, audio, sent, kept, units, radii):
    core = lax.axis_index("core")
    found = [normalize(v[...]) for v in (image, text, audio)]
    for k, (unit, radius) in enumerate(found):
        units[k] = unit
        radii[k] = jnp.broadcast_to(radius, radii.shape[1:])
    image_unit, text_unit, audio_unit = (unit for unit, _ in found)
    sent[:rows] = slim(image_unit)
    kept[:rows] = slim(image_unit)
    sent[rows:] = slim(jnp.where(core == 0, audio_unit, text_unit))
    kept[rows:] = slim(jnp.where(core == 0, text_unit, audio_unit))


def pair_kernel(rows, kept, got, images, others):
    core = lax.axis_index("core")
    images[:rows], images[rows:] = ordered(core, kept[:rows], got[:rows])
    others[:rows], others[rows:] = ordered(core, kept[rows:], got[rows:])


def relay_up_kernel(rows, one, two, out):
    core = lax.axis_index("core")
    out[: 2 * rows] = one[...]
    out[2 * rows :] = jnp.where(core == 0, two[:rows], two[rows:])


def below_kernel(rows, one, two, more, out):
    out[: 2 * rows] = one[...]
    out[2 * rows : 4 * rows] = two[...]
    out[4 * rows :] = more[...]


def folded_rows(e, width):
    folded = sum(e[:, j : j + 128] for j in range(0, width, 128))
    return jnp.sum(folded.T, axis=0, keepdims=True)


def score_kernel(rows, pair, below, above, others, images, exps, row_sums, column_sums):
    at = position()
    count, width = images.shape[0], others.shape[0]
    two = 2 * rows
    images[:two] = pair[...]
    for k in range(3):
        images[(k + 1) * two : (k + 2) * two] = above[k * two : (k + 1) * two]
        images[(7 - k) * two : (8 - k) * two] = below[k * two : (k + 1) * two]
    images[4 * two : 4 * two + rows], images[4 * two + rows : 5 * two] = ordered(
        at[0], below[3 * two :], above[3 * two :]
    )
    columns = other_ids(at, width, rows)
    total = jnp.zeros((1, width), jnp.float32)
    matched = jnp.zeros((1, 1), jnp.float32)
    for m in range(0, count, CHUNK):
        s = logit_scale * dot(images[m : m + CHUNK], others[...], ((1,), (1,)))
        e = jnp.exp(s - logit_scale)
        exps[m : m + CHUNK] = e
        row_sums[:, m : m + CHUNK] = folded_rows(e, width)
        total = total + jnp.sum(e, axis=0, keepdims=True)
        hit = image_ids(at, m, CHUNK, rows) == columns
        found = jnp.sum(jnp.where(hit, s, 0.0), axis=0, keepdims=True)
        matched = matched + jnp.sum(found, axis=1, keepdims=True)
    column_sums[...] = total
    row_sums[:, count:] = jnp.broadcast_to(matched, (1, 128))


def turned(values, lanes):
    n = values.shape[1]
    return pltpu.roll(jnp.broadcast_to(values, (8, n)), (n - lanes) % n, 1)[:1]


def turned_rows(got, steps, rows):
    n = got.shape[1] - 128
    return jnp.concatenate([turned(got[:, :n], steps * 2 * rows % n), got[:, n:]], axis=1)


def row_near_kernel(rows, own, below, above, lower, three):
    both = own[...] + turned_rows(below[...], 1, rows)
    lower[...] = both
    three[...] = both + turned_rows(above[...], -1, rows)


def column_near_kernel(rows, own, got1, got2, got3, out):
    step = own.shape[1] // 4
    for b in range(0, own.shape[1], step):
        total = own[:, b : b + step]
        for k, got in ((1, got1), (2, got2), (3, got3)):
            total = total + turned(got[:, b : b + step], step - 2 * rows * k)
        out[:, b : b + step] = total


def sum_log(values):
    return jnp.sum(jnp.log(values), axis=1, keepdims=True)


def other_kernel(rows, exps, images, three, below, above, line, got1, got2, got3, *outs):
    weights, row_logs, column_logs, out = outs
    at = position()
    count, width = exps.shape
    step = width // 4
    row_all = three[...] + turned_rows(below[...], 3, rows) + turned_rows(above[...], -3, rows)
    row_total, matched = row_all[:, :count], row_all[:, count : count + 1]
    column_total = line[...]
    for k, got in ((1, got1), (2, got2), (3, got3)):
        column_total = column_total + turned(got[...], width - step * k)
    columns = other_ids(at, width, rows)
    by_column = 1.0 / column_total
    for m in range(0, count, CHUNK):
        by_row = 1.0 / row_total[:, m : m + CHUNK]
        by_row = jnp.broadcast_to(by_row, (CHUNK, CHUNK)).T[:, :1]
        hit = image_ids(at, m, CHUNK, rows) == columns
        e = exps[m : m + CHUNK]
        weights[m : m + CHUNK] = slim(e * by_row + e * by_column - jnp.where(hit, 2.0, 0.0))
    logs = sum_log(row_total) - 2.0 * matched
    row_logs[...] = jnp.broadcast_to(logs, row_logs.shape)
    column_logs[...] = jnp.broadcast_to(sum_log(column_total), column_logs.shape)
    other_part(weights, images, 1, logs, out)


def other_part(weights, images, b, logs, out):
    step = weights.shape[1] // 4
    out[:step] = slim(dot(weights[:, b * step : (b + 1) * step], images[...], ((0,), (0,))))
    out[step:] = pieces(logs, images.shape[1])


def rest_kernel(rows, weights, images, row_logs, base, out2, out3):
    step = weights.shape[1] // 4
    for b, out in ((3, out3), (2, out2)):
        other_part(weights, images, b, row_logs[:, :1], out)
    base[...] = dot(weights[:, :step], images[...], ((0,), (0,)))


def image_kernel(rows, weights, others, column_logs, sent, kept):
    core = lax.axis_index("core")
    two = 2 * rows

    def part(p, n=1):
        return dot(weights[p * two : (p + n) * two], others[...], ((1,), (0,)))

    own, upper, lower = part(0), part(1, 4), part(5, 3)
    opposite = upper[3 * two :]
    own_mine, own_other = ordered(core, own[:rows], own[rows:])
    far_mine, far_other = ordered(core, opposite[:rows], opposite[rows:])
    sent[:rows] = slim(own_other)
    sent[rows : 7 * rows] = slim(upper[: 3 * two])
    sent[7 * rows : 8 * rows] = slim(far_other)
    sent[8 * rows :] = pieces(column_logs[:, :1], others.shape[1])
    kept[:rows] = own_mine
    for k in range(3):
        kept[rows + k * two : rows + (k + 1) * two] = lower[(2 - k) * two : (3 - k) * two]
    kept[7 * rows :] = far_mine


def chip_kernel(rows, kept, got, column_logs, near, sent, logs):
    near[...] = kept[: 5 * rows] + wide(got[: 5 * rows])
    sent[: 3 * rows] = slim(kept[5 * rows :] + wide(got[5 * rows : 8 * rows]))
    both = column_logs[:, :1] + whole(got[8 * rows :])
    sent[3 * rows :] = pieces(both, kept.shape[1])
    logs[...] = jnp.broadcast_to(both, logs.shape)


def relay_kernel(rows, near, got, logs, one, two):
    pair = 2 * rows
    core = lax.axis_index("core")
    width = near.shape[1]
    one[:pair] = slim(near[rows : rows + pair] + wide(got[:pair]))
    far = wide(got[pair : pair + rows])
    two[:rows] = slim(near[rows + pair : 2 * pair] + jnp.where(core == 0, far, 0.0))
    two[rows:pair] = slim(near[2 * pair :] + jnp.where(core == 0, 0.0, far))
    theirs = whole(got[pair + rows :])
    one[pair:] = pieces(logs[:, :1] + theirs, width)
    two[pair:] = pieces(logs[:, :1] + jnp.where(core == 0, theirs, 0.0), width)


def line_kernel(rows, base, got1, got2, got3, row_logs, kept, logs, out1, out2, out3):
    pair = 2 * rows
    bundle = base.shape[0]
    both = row_logs[:, :1] + whole(got1[bundle:]) + whole(got2[bundle:]) + whole(got3[bundle:])
    note = pieces(both, base.shape[1])
    for k, out in ((1, out1), (3, out3), (2, out2), (0, kept)):
        at = slice(k * pair, (k + 1) * pair)
        part = base[at] + wide(got1[at]) + wide(got2[at]) + wide(got3[at])
        if k:
            out[:pair] = slim(part)
            out[pair:] = note
        else:
            out[...] = part
    logs[...] = jnp.broadcast_to(both, logs.shape)


def gather_kernel(rows, line, got1, got2, got3, near, one, two, row_logs, column_logs, *outs):
    sent, kept, logs = outs
    pair = 2 * rows
    core = lax.axis_index("core")
    other = line[...] + wide(got1[:pair]) + wide(got2[:pair]) + wide(got3[:pair])
    both = wide(one[:pair]) + wide(two[:pair])
    mine, partners = ordered(core, both[:rows], both[rows:])
    kept[:rows] = near[:rows] + mine
    sent[:rows] = slim(partners)
    mine, partners = ordered(core, other[:rows], other[rows:])
    kept[rows:] = mine
    sent[rows:pair] = slim(partners)
    total = row_logs[:, :1] + whole(got1[pair:]) + whole(got2[pair:]) + whole(got3[pair:])
    total = total + whole(one[pair:]) + whole(two[pair:])
    total = total + jnp.where(core == 0, column_logs[:, :1], 0.0)
    sent[pair:] = pieces(total, line.shape[1])
    logs[...] = jnp.broadcast_to(total, logs.shape)


def end_kernel(rows, kept, got, logs, units, radii, image_out, text_out, audio_out, loss):
    core = lax.axis_index("core")
    sums = (kept[:rows] + wide(got[:rows]), *ordered(core, kept[rows:], wide(got[rows : 2 * rows])))
    for k, (total, out) in enumerate(zip(sums, (image_out, text_out, audio_out))):
        unit, radius = units[k], radii[k][:, :1]
        grad = logit_scale * total
        inner = jnp.sum(unit * grad, axis=-1, keepdims=True)
        out[...] = (grad - unit * inner) / radius
    total = logs[:, :1] + whole(got[2 * rows :])
    loss[...] = total / (4.0 * 256 * rows) + logit_scale


def step(image, text, audio):
    rows, width = image.shape
    pair, bundle = 2 * rows, 8 * rows
    bf16, f32 = jnp.bfloat16, jnp.float32

    def local(kernel, arrays, *shapes, **options):
        def bound(*refs):
            kernel(rows, *refs)

        return call(bound, len(arrays), *shapes, **options)(*arrays)

    two = ((pair, width), bf16)
    sent, kept, units, radii = local(
        begin_kernel,
        (image, text, audio),
        two,
        two,
        ((3, rows, width), f32),
        ((3, rows, 128), f32),
        outside=True,
    )
    got = swap(sent)
    image_pair, other_pair = local(pair_kernel, (kept, got), two, two)

    near = {k: along_first(other_pair, k) for k in (1, 3, 2)}
    ups = {k: up(image_pair, k) for k in (1, 2)}
    line = jnp.concatenate([other_pair, near[1], near[2], near[3]])
    far = {k: along_second(line, k) for k in (1, 3, 2)}
    (more,) = local(relay_up_kernel, (ups[1], ups[2]), ((3 * rows, width), bf16))
    more = up(more, 2)
    (below,) = local(below_kernel, (ups[1], ups[2], more), ((7 * rows, width), bf16))
    above = swap(below)
    others = jnp.concatenate([line, far[1], far[2], far[3]])

    count, across = 8 * pair, others.shape[0]
    row_shape, column_shape = ((1, count + 128), f32), ((1, across), f32)
    images, exps, row_sums, column_sums = local(
        score_kernel,
        (image_pair, below, above, others),
        ((count, width), bf16),
        ((count, across), f32),
        row_shape,
        column_shape,
    )
    rows_below, rows_above = up(row_sums, 1), up(row_sums, -1)
    lower, three = local(row_near_kernel, (row_sums, rows_below, rows_above), row_shape, row_shape)
    rows_below, rows_above = up(three, 3), up(lower, -3)
    got = {k: along_first(column_sums, k) for k in (1, 3, 2)}
    (columns,) = local(column_near_kernel, (column_sums, got[1], got[2], got[3]), column_shape)
    got = {k: along_second(columns, k) for k in (1, 3, 2)}

    packet, log = ((bundle + NOTE, width), bf16), ((1, 128), f32)
    weights, row_logs, column_logs, first = local(
        other_kernel,
        (exps, images, three, rows_below, rows_above, columns, got[1], got[2], got[3]),
        ((count, across), bf16),
        log,
        log,
        packet,
    )
    base, *packets = local(
        rest_kernel, (weights, images, row_logs), ((bundle, width), f32), packet, packet
    )
    packets = [first, *packets]
    seconds = {k: along_second(packets[k - 1], -k) for k in (1, 3, 2)}

    sent, kept = local(image_kernel, (weights, others, column_logs), packet, ((bundle, width), f32))
    got = swap(sent)
    around, sent, column_logs = local(
        chip_kernel,
        (kept, got, column_logs),
        ((5 * rows, width), f32),
        ((3 * rows + NOTE, width), bf16),
        log,
    )
    more = up(sent, -2)
    packet = ((pair + NOTE, width), bf16)
    one, two = local(relay_kernel, (around, more, column_logs), packet, packet)
    one, two = up(one, -1), up(two, -2)

    kept, row_logs, *packets = local(
        line_kernel,
        (base, seconds[1], seconds[2], seconds[3], row_logs),
        ((pair, width), f32),
        log,
        packet,
        packet,
        packet,
    )
    firsts = {k: along_first(packets[k - 1], -k) for k in (1, 3, 2)}

    sent, kept, logs = local(
        gather_kernel,
        (kept, firsts[1], firsts[2], firsts[3], around, one, two, row_logs, column_logs),
        packet,
        ((pair, width), f32),
        log,
    )
    got = swap(sent)
    shape = ((rows, width), f32)
    image_grad, text_grad, audio_grad, loss = local(
        end_kernel, (kept, got, logs, units, radii), shape, shape, shape, ((1, 1), f32), last=True
    )
    return image_grad, text_grad, audio_grad, loss.reshape(())


def solution(mesh):
    split = Mesh(mesh.devices.reshape(2, 2, 8, 2, 4), AXES)
    image_spec, other_spec = P(COL_ROW, None), P(AXES, None)
    return jax.shard_map(
        step,
        mesh=split,
        in_specs=(image_spec, other_spec, other_spec),
        out_specs=(image_spec, other_spec, other_spec, P()),
        check_vma=False,
    )
```

```python
import math

import jax
import jax.numpy as jnp
from jax import lax
from jax.experimental import pallas as pl
from jax.experimental.pallas import tpu as pltpu
from jax.sharding import Mesh
from jax.sharding import PartitionSpec as P

AXES = ("y_lo", "core", "z", "y_hi", "x")
COL_ROW = ("z", "y_hi", "x", "y_lo", "core")

logit_scale = 20.0
epsilon = 1e-06
NOTE = 8
CHUNK = 128


def place(core, x, y, z):
    return (((y % 4 % 2 * 2 + core % 2) * 8 + z % 8) * 2 + y % 4 // 2) * 4 + x % 4


def send(array, move):
    pairs = [
        (place(core, x, y, z), place(*move(core, x, y, z)))
        for core in range(2)
        for x in range(4)
        for y in range(4)
        for z in range(8)
    ]
    return lax.ppermute(array, AXES, pairs)


def swap(array):
    return send(array, lambda core, x, y, z: (1 - core, x, y, z))


def along_first(array, k):
    return send(array, lambda core, x, y, z: (core, x, y + k, z) if core else (core, x + k, y, z))


def along_second(array, k):
    return send(array, lambda core, x, y, z: (core, x + k, y, z) if core else (core, x, y + k, z))


def up(array, k):
    return send(array, lambda core, x, y, z: (core, x, y, z - k if core else z + k))


def call(kernel, count, *shapes, last=False, outside=False):
    def space(shape, dtype):
        return jax.ShapeDtypeStruct(shape, dtype) if last else pltpu.VMEM(shape, dtype)

    made = pl.pallas_call(
        kernel,
        out_shape=tuple(space(s, d) for s, d in shapes),
        in_specs=[pl.BlockSpec(memory_space=pltpu.VMEM)] * count,
        out_specs=tuple(pl.BlockSpec(memory_space=pltpu.VMEM) for _ in shapes),
        compiler_params=pltpu.CompilerParams(vmem_limit_bytes=20 * 1024 * 1024),
    )

    def run(*arrays):
        kept_in = pltpu.HBM if outside else pltpu.VMEM
        return made(*(pltpu.with_memory_space_constraint(a, kept_in) for a in arrays))

    return run


def wide(values):
    return values.astype(jnp.float32)


def slim(values):
    return values.astype(jnp.bfloat16)


def normalize(values):
    widened = wide(values)
    radius = jnp.sqrt(jnp.sum(widened * widened, axis=-1, keepdims=True) + epsilon)
    return (widened / radius, radius)


def dot(left, right, contract):
    return lax.dot_general(left, right, (contract, ((), ())), preferred_element_type=jnp.float32)


def pieces(value, width):
    value = jnp.broadcast_to(value, (NOTE, width))
    high = wide(slim(value))
    rest = value - high
    middle = wide(slim(rest))
    lane = lax.broadcasted_iota(jnp.int32, (NOTE, width), 1)
    split = jnp.where(lane == 0, high, jnp.where(lane == 1, middle, rest - middle))
    return slim(jnp.where(lane < 3, split, 0.0))


def whole(rows):
    return jnp.sum(wide(rows)[:1, :128], axis=1, keepdims=True)


def position():
    core, z, x = lax.axis_index("core"), lax.axis_index("z"), lax.axis_index("x")
    return core, x, lax.axis_index("y_hi") * 2 + lax.axis_index("y_lo"), z


def image_ids(at, first_row, count, rows):
    core, x, y, z = at
    r = first_row + lax.broadcasted_iota(jnp.int32, (count, 1), 0)
    block = r // rows
    at_z = (z + jnp.where(core == 0, block // 2, 8 - block // 2)) % 8
    where = at_z * 32 + y // 2 * 16 + x * 4 + y % 2 * 2 + block % 2
    return where * rows + r % rows


def other_ids(at, first_row, count, rows):
    core, x, y, z = at
    r = first_row + lax.broadcasted_iota(jnp.int32, (1, count), 1)
    block = r // rows
    a, b = block // 2 % 4, block // 8
    at_x = (x - jnp.where(core == 0, a, b) + 4) % 4
    at_y = (y - jnp.where(core == 0, b, a) + 4) % 4
    where = at_y % 2 * 128 + block % 2 * 64 + z * 8 + at_y // 2 * 4 + at_x
    return where * rows + r % rows


def ordered(core, mine, other):
    return jnp.where(core == 0, mine, other), jnp.where(core == 0, other, mine)


def begin_kernel(rows, image, text, audio, sent, kept, units, radii):
    core = lax.axis_index("core")
    found = [normalize(v[...]) for v in (image, text, audio)]
    for k, (unit, radius) in enumerate(found):
        units[k] = unit
        radii[k] = jnp.broadcast_to(radius, radii.shape[1:])
    image_unit, text_unit, audio_unit = (unit for unit, _ in found)
    sent[:rows] = slim(image_unit)
    kept[:rows] = slim(image_unit)
    sent[rows:] = slim(jnp.where(core == 0, audio_unit, text_unit))
    kept[rows:] = slim(jnp.where(core == 0, text_unit, audio_unit))


def pair_kernel(rows, kept, got, images, others):
    core = lax.axis_index("core")
    images[:rows], images[rows:] = ordered(core, kept[:rows], got[:rows])
    others[:rows], others[rows:] = ordered(core, kept[rows:], got[rows:])


def relay_up_kernel(rows, one, two, out):
    core = lax.axis_index("core")
    out[: 2 * rows] = one[...]
    out[2 * rows :] = jnp.where(core == 0, two[:rows], two[rows:])


def below_kernel(rows, one, two, more, out):
    out[: 2 * rows] = one[...]
    out[2 * rows : 4 * rows] = two[...]
    out[4 * rows :] = more[...]


def folded_rows(e, width):
    folded = sum(e[:, j : j + 128] for j in range(0, width, 128))
    return jnp.sum(folded.T, axis=0, keepdims=True)


def score_kernel(rows, pair, below, above, others, images, exps, row_sums, column_sums):
    at = position()
    count, width = images.shape[0], others.shape[0]
    two = 2 * rows
    images[:two] = pair[...]
    for k in range(3):
        images[(k + 1) * two : (k + 2) * two] = above[k * two : (k + 1) * two]
        images[(7 - k) * two : (8 - k) * two] = below[k * two : (k + 1) * two]
    images[4 * two : 4 * two + rows], images[4 * two + rows : 5 * two] = ordered(
        at[0], below[3 * two :], above[3 * two :]
    )
    columns = other_ids(at, 0, width, rows)
    total = jnp.zeros((1, width), jnp.float32)
    matched = jnp.zeros((1, 1), jnp.float32)
    rate = logit_scale / math.log(2.0)
    for m in range(0, count, CHUNK):
        s = dot(images[m : m + CHUNK], others[...], ((1,), (1,)))
        e = jnp.exp2(s * rate - rate)
        exps[m : m + CHUNK] = e
        row_sums[:, m : m + CHUNK] = folded_rows(e, width)
        total = total + jnp.sum(e, axis=0, keepdims=True)
        hit = image_ids(at, m, CHUNK, rows) == columns
        found = jnp.sum(jnp.where(hit, s, 0.0), axis=0, keepdims=True)
        matched = matched + jnp.sum(found, axis=1, keepdims=True)
    column_sums[...] = total
    row_sums[:, count:] = jnp.broadcast_to(logit_scale * matched, (1, 128))


def turned(values, lanes):
    n = values.shape[1]
    return pltpu.roll(jnp.broadcast_to(values, (8, n)), (n - lanes) % n, 1)[:1]


def turned_rows(got, steps, rows):
    n = got.shape[1] - 128
    return jnp.concatenate([turned(got[:, :n], steps * 2 * rows % n), got[:, n:]], axis=1)


def row_near_kernel(rows, own, below, above, lower, three):
    both = own[...] + turned_rows(below[...], 1, rows)
    lower[...] = both
    three[...] = both + turned_rows(above[...], -1, rows)


def column_near_kernel(rows, own, got1, got2, got3, out):
    step = own.shape[1] // 4
    for b in range(0, own.shape[1], step):
        total = own[:, b : b + step]
        for k, got in ((1, got1), (2, got2), (3, got3)):
            total = total + turned(got[:, b : b + step], step - 2 * rows * k)
        out[:, b : b + step] = total


def sum_log(values):
    return jnp.sum(jnp.log(values), axis=1, keepdims=True)


def weigh(rows, exps, row_total, column_total, b, out, at_column=0):
    at = position()
    count, width = exps.shape
    step = width // 4
    here = slice(b * step, (b + 1) * step)
    there = slice(at_column, at_column + step)
    columns = other_ids(at, b * step, step, rows)
    by_column = 1.0 / column_total[:, here]
    for m in range(0, count, CHUNK):
        by_row = 1.0 / row_total[:, m : m + CHUNK]
        by_row = jnp.broadcast_to(by_row, (CHUNK, CHUNK)).T[:, :1]
        hit = image_ids(at, m, CHUNK, rows) == columns
        e = exps[m : m + CHUNK, here]
        out[m : m + CHUNK, there] = slim(e * by_row + e * by_column - jnp.where(hit, 2.0, 0.0))


def other_kernel(rows, exps, images, three, below, above, line, got1, got2, got3, *outs):
    weights, rows_out, columns_out, row_logs, out = outs
    count, width = exps.shape
    step = width // 4
    row_all = three[...] + turned_rows(below[...], 3, rows) + turned_rows(above[...], -3, rows)
    row_total, matched = row_all[:, :count], row_all[:, count : count + 1]
    column_total = line[...]
    for k, got in ((1, got1), (2, got2), (3, got3)):
        column_total = column_total + turned(got[...], width - step * k)
    rows_out[...], columns_out[...] = row_total, column_total
    weigh(rows, exps, row_total, column_total, 1, weights)
    logs = sum_log(row_total) - 2.0 * matched
    row_logs[...] = jnp.broadcast_to(logs, row_logs.shape)
    other_part(weights[...], images, logs, out)


def other_part(weights, images, logs, out):
    step = weights.shape[1]
    out[:step] = slim(dot(weights, images[...], ((0,), (0,))))
    out[step:] = pieces(logs, images.shape[1])


def rest_kernel(rows, exps, images, first, row_total, column_total, row_logs, *outs):
    weights, base, out2, out3 = outs
    step = exps.shape[1] // 4
    row_total, column_total = row_total[...], column_total[...]
    for b, out in ((3, out3), (2, out2)):
        weigh(rows, exps, row_total, column_total, b, weights, b * step)
        other_part(weights[:, b * step : (b + 1) * step], images, row_logs[:, :1], out)
    weigh(rows, exps, row_total, column_total, 0, weights)
    base[...] = dot(weights[:, :step], images[...], ((0,), (0,)))
    weights[:, step : 2 * step] = first[...]


def image_kernel(rows, weights, others, column_total, sent, kept, logs):
    core = lax.axis_index("core")
    two = 2 * rows
    part = dot(weights[: 5 * two], others[...], ((1,), (0,)))
    mine, other = ordered(core, part[:rows], part[rows:two])
    kept[:rows] = mine
    sent[:rows] = slim(other)
    sent[rows : 7 * rows] = slim(part[two : 4 * two])
    mine, other = ordered(core, part[4 * two : 9 * rows], part[9 * rows :])
    kept[rows:] = mine
    sent[7 * rows : 8 * rows] = slim(other)
    total = sum_log(column_total[...])
    sent[8 * rows :] = pieces(total, others.shape[1])
    logs[...] = jnp.broadcast_to(total, logs.shape)


def lower_kernel(rows, weights, others, kept, out):
    two = 2 * rows
    part = dot(weights[5 * two :], others[...], ((1,), (0,)))
    out[:rows] = kept[:rows]
    for k in range(3):
        out[rows + k * two : rows + (k + 1) * two] = part[(2 - k) * two : (3 - k) * two]
    out[7 * rows :] = kept[rows:]


def chip_kernel(rows, kept, got, column_logs, near, sent, logs):
    near[...] = kept[: 5 * rows] + wide(got[: 5 * rows])
    sent[: 3 * rows] = slim(kept[5 * rows :] + wide(got[5 * rows : 8 * rows]))
    both = column_logs[:, :1] + whole(got[8 * rows :])
    sent[3 * rows :] = pieces(both, kept.shape[1])
    logs[...] = jnp.broadcast_to(both, logs.shape)


def relay_kernel(rows, near, got, logs, one, two):
    pair = 2 * rows
    core = lax.axis_index("core")
    width = near.shape[1]
    one[:pair] = slim(near[rows : rows + pair] + wide(got[:pair]))
    far = wide(got[pair : pair + rows])
    two[:rows] = slim(near[rows + pair : 2 * pair] + jnp.where(core == 0, far, 0.0))
    two[rows:pair] = slim(near[2 * pair :] + jnp.where(core == 0, 0.0, far))
    theirs = whole(got[pair + rows :])
    one[pair:] = pieces(logs[:, :1] + theirs, width)
    two[pair:] = pieces(logs[:, :1] + jnp.where(core == 0, theirs, 0.0), width)


def line_kernel(rows, base, got1, got2, got3, row_logs, kept, logs, out1, out2, out3):
    pair = 2 * rows
    bundle = base.shape[0]
    both = row_logs[:, :1] + whole(got1[bundle:]) + whole(got2[bundle:]) + whole(got3[bundle:])
    note = pieces(both, base.shape[1])
    for k, out in ((1, out1), (3, out3), (2, out2), (0, kept)):
        at = slice(k * pair, (k + 1) * pair)
        part = base[at] + wide(got1[at]) + wide(got2[at]) + wide(got3[at])
        if k:
            out[:pair] = slim(part)
            out[pair:] = note
        else:
            out[...] = part
    logs[...] = jnp.broadcast_to(both, logs.shape)


def gather_kernel(rows, line, got1, got2, got3, near, one, two, row_logs, column_logs, *outs):
    sent, kept, logs = outs
    pair = 2 * rows
    core = lax.axis_index("core")
    other = line[...] + wide(got1[:pair]) + wide(got2[:pair]) + wide(got3[:pair])
    both = wide(one[:pair]) + wide(two[:pair])
    mine, partners = ordered(core, both[:rows], both[rows:])
    kept[:rows] = near[:rows] + mine
    sent[:rows] = slim(partners)
    mine, partners = ordered(core, other[:rows], other[rows:])
    kept[rows:] = mine
    sent[rows:pair] = slim(partners)
    total = row_logs[:, :1] + whole(got1[pair:]) + whole(got2[pair:]) + whole(got3[pair:])
    total = total + whole(one[pair:]) + whole(two[pair:])
    total = total + jnp.where(core == 0, column_logs[:, :1], 0.0)
    sent[pair:] = pieces(total, line.shape[1])
    logs[...] = jnp.broadcast_to(total, logs.shape)


def end_kernel(rows, kept, got, logs, units, radii, image_out, text_out, audio_out, loss):
    core = lax.axis_index("core")
    sums = (kept[:rows] + wide(got[:rows]), *ordered(core, kept[rows:], wide(got[rows : 2 * rows])))
    for k, (total, out) in enumerate(zip(sums, (image_out, text_out, audio_out))):
        unit, radius = units[k], radii[k][:, :1]
        grad = logit_scale * total
        inner = jnp.sum(unit * grad, axis=-1, keepdims=True)
        out[...] = (grad - unit * inner) / radius
    total = logs[:, :1] + whole(got[2 * rows :])
    loss[...] = total / (4.0 * 256 * rows) + logit_scale


def step(image, text, audio):
    rows, width = image.shape
    pair, bundle = 2 * rows, 8 * rows
    bf16, f32 = jnp.bfloat16, jnp.float32

    def local(kernel, arrays, *shapes, **options):
        def bound(*refs):
            kernel(rows, *refs)

        return call(bound, len(arrays), *shapes, **options)(*arrays)

    two = ((pair, width), bf16)
    sent, kept, units, radii = local(
        begin_kernel,
        (image, text, audio),
        two,
        two,
        ((3, rows, width), f32),
        ((3, rows, 128), f32),
        outside=True,
    )
    got = swap(sent)
    image_pair, other_pair = local(pair_kernel, (kept, got), two, two)

    near = {k: along_first(other_pair, k) for k in (1, 3, 2)}
    ups = {k: up(image_pair, k) for k in (1, 2)}
    line = jnp.concatenate([other_pair, near[1], near[2], near[3]])
    far = {k: along_second(line, k) for k in (1, 3, 2)}
    (more,) = local(relay_up_kernel, (ups[1], ups[2]), ((3 * rows, width), bf16))
    more = up(more, 2)
    (below,) = local(below_kernel, (ups[1], ups[2], more), ((7 * rows, width), bf16))
    above = swap(below)
    others = jnp.concatenate([line, far[1], far[2], far[3]])

    count, across = 8 * pair, others.shape[0]
    row_shape, column_shape = ((1, count + 128), f32), ((1, across), f32)
    images, exps, row_sums, column_sums = local(
        score_kernel,
        (image_pair, below, above, others),
        ((count, width), bf16),
        ((count, across), f32),
        row_shape,
        column_shape,
    )
    rows_below, rows_above = up(row_sums, 1), up(row_sums, -1)
    lower, three = local(row_near_kernel, (row_sums, rows_below, rows_above), row_shape, row_shape)
    rows_below, rows_above = up(three, 3), up(lower, -3)
    got = {k: along_first(column_sums, k) for k in (1, 3, 2)}
    (columns,) = local(column_near_kernel, (column_sums, got[1], got[2], got[3]), column_shape)
    got = {k: along_second(columns, k) for k in (1, 3, 2)}

    packet, log = ((bundle + NOTE, width), bf16), ((1, 128), f32)
    first, row_total, column_total, row_logs, packet1 = local(
        other_kernel,
        (exps, images, three, rows_below, rows_above, columns, got[1], got[2], got[3]),
        ((count, across // 4), bf16),
        ((1, count), f32),
        column_shape,
        log,
        packet,
    )
    weights, base, *packets = local(
        rest_kernel,
        (exps, images, first, row_total, column_total, row_logs),
        ((count, across), bf16),
        ((bundle, width), f32),
        packet,
        packet,
    )
    packets = [packet1, *packets]
    seconds = {k: along_second(packets[k - 1], -k) for k in (1, 3, 2)}

    sent, kept, column_logs = local(
        image_kernel, (weights, others, column_total), packet, ((pair, width), f32), log
    )
    got = swap(sent)
    (kept,) = local(lower_kernel, (weights, others, kept), ((bundle, width), f32))
    around, sent, column_logs = local(
        chip_kernel,
        (kept, got, column_logs),
        ((5 * rows, width), f32),
        ((3 * rows + NOTE, width), bf16),
        log,
    )
    more = up(sent, -2)
    packet = ((pair + NOTE, width), bf16)
    one, two = local(relay_kernel, (around, more, column_logs), packet, packet)
    one, two = up(one, -1), up(two, -2)

    kept, row_logs, *packets = local(
        line_kernel,
        (base, seconds[1], seconds[2], seconds[3], row_logs),
        ((pair, width), f32),
        log,
        packet,
        packet,
        packet,
    )
    firsts = {k: along_first(packets[k - 1], -k) for k in (1, 3, 2)}

    sent, kept, logs = local(
        gather_kernel,
        (kept, firsts[1], firsts[2], firsts[3], around, one, two, row_logs, column_logs),
        packet,
        ((pair, width), f32),
        log,
    )
    got = swap(sent)
    shape = ((rows, width), f32)
    image_grad, text_grad, audio_grad, loss = local(
        end_kernel, (kept, got, logs, units, radii), shape, shape, shape, ((1, 1), f32), last=True
    )
    return image_grad, text_grad, audio_grad, loss.reshape(())


def solution(mesh):
    split = Mesh(mesh.devices.reshape(2, 2, 8, 2, 4), AXES)
    image_spec, other_spec = P(COL_ROW, None), P(AXES, None)
    return jax.shard_map(
        step,
        mesh=split,
        in_specs=(image_spec, other_spec, other_spec),
        out_specs=(image_spec, other_spec, other_spec, P()),
        check_vma=False,
    )
```
